32 devices in a mesh: dp: 4 (over y, core), expert: 4 (over z), tensor: 2 (over x).
Axes of the slice: x: 2, y: 2, z: 4, core: 2. Of those that a mesh axis runs over, the one named last changes fastest.
Arguments:
- tokens: bfloat16 [96, 7168], P('expert', 'tensor'), may hold values from -6 to 6
- expert_ids: int32 [96, 8], P('expert'), may hold values from 0 to 63, all different within a row; in each aligned block of 24 rows (0 to 23, 24 to 47, ...) at most 4 rows name the same one
- gate_weights: float32 [96, 8], P('expert'), may hold values from 0.1 to 1
- w_gate: bfloat16 [64, 7168, 1024], P('expert', 'tensor', 'dp'), may hold values from -0.0625 to 0.0625
- w_up: bfloat16 [64, 7168, 1024], P('expert', 'tensor', 'dp'), may hold values from -0.0625 to 0.0625
- w_down: bfloat16 [64, 1024, 7168], P('expert', 'dp', 'tensor'), may hold values from -0.1875 to 0.1875
Outputs:
- mixed: bfloat16 [96, 7168], P('expert', 'tensor')
The draws below stay inside these ranges and needn't reach their ends.
Inputs may be any that keep to these rules, and one draw needn't show every extreme that they name: `expert_ids`: each row names 8 different experts. Among the rows of one index of the expert axis (aligned blocks of 24 rows) no expert is named more than 4 times, and in some block one expert is named exactly 4 times.
All inputs are finite; a program needn't handle non-finite values.
Results may differ from the reference program's by a relative error of at most 0.0049.
Values may be sent and summed in bfloat16 or wider, within the bound.
A program may use at most 128 MiB of HBM per device.

```python
import math
import jax
import jax.numpy as jnp
import numpy as np
from jax import lax

D = 7168
FF = 1024
TOP = 8
EXPERTS = 64
T_DEV = 24
CAP = 4
TOKENS = 96
N_EXPERT = 4


def level_of(rng, dims, cuts, smallest, high):
    def one(axis_at, blocks):
        heights = jax.random.uniform(jax.random.fold_in(jax.random.fold_in(rng, 6), axis_at), (blocks,), jnp.float32, smallest / len(cuts), high / len(cuts))
        return jnp.repeat(jnp.exp(heights), dims[axis_at] // blocks).reshape((-1,) + (1,) * (len(dims) - axis_at - 1))

    gain = one(*cuts[0])
    for cut in cuts[1:]:
        gain = gain * one(*cut)
    return gain


def shared_out(key, own, number, rows, count, top, bound, slope):
    ranking = jax.random.permutation(key, count)
    packed, ordinary = shares(count, rows * top, bound, slope, True), shares(count, rows * top, bound, slope, False)
    places = jnp.arange(count)

    def named(lengths, turn):
        used = int((lengths > 0).sum())
        fixed = max(1, used // 4)
        shifted = fixed + (places - fixed + turn * (used - fixed)) % max(1, count - fixed)
        return jnp.zeros((count,), jnp.int32).at[ranking[jnp.where(places < fixed, places, shifted)]].set(jnp.asarray(lengths, jnp.int32))

    lengths = jnp.where(number % 4 == 0, named(packed, number // 4), named(ordinary, number - number // 4 - 1))
    mixed = jax.random.permutation(jax.random.fold_in(own, 3), count)
    giver, taker = mixed[0:count // 2 * 2:2], mixed[1:count // 2 * 2:2]
    room = jnp.minimum(lengths[giver] - 1, bound - lengths[taker]) // 2
    room = jnp.where((giver == ranking[0]) | (taker == ranking[0]) | (lengths[taker] == 0), 0, jnp.maximum(room, 0))
    shifted = jax.random.randint(jax.random.fold_in(own, 4), (count // 2,), 0, 1 << 20) % (room + 1)
    lengths = lengths.at[giver].add(-shifted).at[taker].add(shifted)
    members = jnp.searchsorted(jnp.cumsum(lengths), jnp.arange(rows * top), side="right").astype(jnp.int32)
    table = members.reshape(top, rows).T
    table = table[jax.random.permutation(jax.random.fold_in(own, 1), rows)]
    turn = jax.random.randint(jax.random.fold_in(own, 2), (rows, 1), 0, top)
    return jnp.take_along_axis(table, (jnp.arange(top)[None, :] + turn) % top, axis=1)


def shares(count, total, most, skew, full):
    portions = [(1 << 20) // math.isqrt(standing ** skew) + 1 for standing in range(1, count + 1)]
    largest = most if full else min(most, max(-(-total // count), total * portions[0] // sum(portions)))
    least = 1 if total - largest >= count - 1 else 0
    given, spare = [largest] + [least] * (count - 1), total - largest - least * (count - 1)
    while spare > 0:
        candidates = [i for i in range(1, count) if given[i] < largest] or [i for i in range(1, count) if given[i] < most]
        mass, remaining = sum([portions[i] for i in candidates]), spare
        for i in candidates:
            addition = min(most - given[i], max(1, remaining * portions[i] // mass), spare)
            given[i] = given[i] + addition
            spare = spare - addition
    return np.array(given)


def noise(key, shape, deviation, most, shards=(), held_as=jnp.bfloat16):
    drawn = jax.random.normal(key, shape, jnp.float32) * deviation
    if len(shards) > 0:
        drawn = level_of(key, shape, shards, -0.22, 0.18) * drawn
    return jnp.clip(drawn, min=-most, max=most).astype(held_as)


def setup_inputs(seed: int = 0) -> dict:
    key_of = jax.random.split(jax.random.key(seed), 7)
    tokens = noise(key_of[0], (TOKENS, D), 1.0, 6.0, ((0, 4), (1, 2)))
    expert_ids_keys = jax.random.split(jax.random.fold_in(key_of[1], 1), TOKENS // T_DEV)
    expert_ids_turns = jax.random.permutation(jax.random.fold_in(key_of[1], 3), TOKENS // T_DEV)
    expert_ids = jax.vmap(lambda own, number: shared_out(jax.random.fold_in(key_of[1], 2), own, number, T_DEV, EXPERTS, TOP, CAP, 2))(expert_ids_keys, expert_ids_turns).reshape((TOKENS, TOP))
    gate_weights = jnp.clip(jnp.exp(math.log(1.0) - 2.3025851 * jax.random.uniform(key_of[2], (TOKENS, TOP), jnp.float32) ** level_of(key_of[2], (TOKENS, TOP), ((0, 4),), -0.2, 0.2)), 0.1, 1.0)
    w_gate = noise(key_of[3], (EXPERTS, D, FF), D ** -0.5, 0.0625, ((0, 4), (1, 2), (2, 4)))
    w_up = noise(key_of[4], (EXPERTS, D, FF), D ** -0.5, 0.0625, ((0, 4), (1, 2), (2, 4)))
    w_down = noise(key_of[5], (EXPERTS, FF, D), FF ** -0.5, 0.1875, ((0, 4), (1, 4), (2, 2)))
    return {"tokens": tokens, "expert_ids": expert_ids, "gate_weights": gate_weights, "w_gate": w_gate, "w_up": w_up, "w_down": w_down}


def reference(tokens, expert_ids, gate_weights, w_gate, w_up, w_down):
    assignments = TOKENS * TOP
    slots_per_expert = N_EXPERT * CAP
    flat_ids = expert_ids.reshape(-1).astype(jnp.int32)
    sort_order = jnp.argsort(flat_ids, stable=True).astype(jnp.int32)
    sorted_ids = flat_ids[sort_order]
    totals = jnp.sum((flat_ids[:, None] == jnp.arange(EXPERTS, dtype=jnp.int32)[None, :]).astype(jnp.int32), axis=0)
    offsets = (jnp.cumsum(totals) - totals).astype(jnp.int32)
    slot_rank = jnp.arange(assignments, dtype=jnp.int32) - offsets[sorted_ids]
    slot_table = jnp.full((EXPERTS * slots_per_expert,), assignments, jnp.int32)
    slot_table = slot_table.at[sorted_ids * slots_per_expert + slot_rank].set(sort_order)
    slot_table = slot_table.reshape(EXPERTS, slots_per_expert)
    padded_tokens = jnp.concatenate([tokens, jnp.zeros((1, D), tokens.dtype)], axis=0)
    padded_weights = jnp.concatenate([gate_weights.reshape(-1), jnp.zeros((1,), gate_weights.dtype)])

    def one_expert(running, inputs):
        entries, gate_matrix, up_matrix, down_matrix = inputs
        token_rows = (entries // TOP).astype(jnp.int32)
        chosen = padded_tokens[token_rows]
        gate_pre = jnp.dot(chosen, gate_matrix, preferred_element_type=jnp.float32)
        up_pre = jnp.dot(chosen, up_matrix, preferred_element_type=jnp.float32)
        hidden = (jax.nn.silu(gate_pre) * up_pre).astype(jnp.bfloat16)
        expert_out = jnp.dot(hidden, down_matrix, preferred_element_type=jnp.float32)
        running = running.at[token_rows].add(expert_out * padded_weights[entries][:, None])
        return running, None

    initial = jnp.zeros((TOKENS + 1, D), jnp.float32)
    running, _ = lax.scan(one_expert, initial, (slot_table, w_gate, w_up, w_down))
    return running[:TOKENS].astype(jnp.bfloat16)
```

```python
import functools

import jax
import jax.numpy as jnp
from jax import lax
from jax.experimental import pallas as pl
from jax.experimental.pallas import tpu as pltpu
from jax.sharding import PartitionSpec as P

CAP = 4
LANES = 128
WEIGHT_VMEM = 57_500_000
VMEM_LIMIT = 67_043_328
DOWN_SLOTS = 8
HIDDEN_LAG = 4
MESH = pl.DeviceIdType.MESH
BF16, F32, I32 = jnp.bfloat16, jnp.float32, jnp.int32


def layer_kernel(
    cfg, tok_hbm, ids_hbm, gw_hbm, wg_hbm, wu_hbm, wd_hbm, out_ref,
    wg, wu, wd, tok, ids, gw, table, scale, rows_x, snd, rcv, dense,
    rs_buf, rs_recv, ex_send, ex_recv, ag,
    gu_sem, wd_sem, loc_sem, tok_send, tok_recv, rel_send, rel_recv, ids_send, ids_recv, gw_send, gw_recv,
    gu_send, gu_recv, rs_ssem, rs_rsem, ex_ssem, ex_rsem, ag_ssem, ag_rsem,
):
    n_e, n_d, n_t = cfg["n_e"], cfg["n_d"], cfg["n_t"]
    experts, width, hid = cfg["experts"], cfg["width"], cfg["hid"]
    t_dev, t_pad, top = cfg["t_dev"], cfg["t_pad"], cfg["top"]
    ng, nd, chunk, chunks = cfg["ng"], cfg["nd"], cfg["chunk"], cfg["chunks"]
    part = chunk // n_d
    slots = n_e * CAP
    all_slots = experts * slots
    me_e, me_d, me_t = lax.axis_index("expert"), lax.axis_index("dp"), lax.axis_index("tensor")

    next_e, next_d = lax.rem(me_e + 1, n_e), lax.rem(me_d + 1, n_d)

    def gate_copy(e, slot):
        return pltpu.make_async_copy(wg_hbm.at[e], wg.at[slot], gu_sem.at[0, slot])

    def up_copy(e, slot):
        return pltpu.make_async_copy(wu_hbm.at[e], wu.at[slot], gu_sem.at[1, slot])

    def down_copy(c, slot):
        cols = pl.ds(c * chunk if isinstance(c, int) else pl.multiple_of(c * chunk, LANES), chunk)
        return pltpu.make_async_copy(wd_hbm.at[:, :, cols], wd.at[slot], wd_sem.at[slot])

    def remote(src, dst, ssem, rsem, **where):
        return pltpu.make_async_remote_copy(
            src_ref=src, dst_ref=dst, send_sem=ssem, recv_sem=rsem, device_id=where, device_id_type=MESH
        )

    own_rows = pl.ds(0, t_dev)
    local = (
        pltpu.make_async_copy(ids_hbm, ids.at[0], loc_sem.at[0]),
        pltpu.make_async_copy(gw_hbm, gw.at[0], loc_sem.at[1]),
        pltpu.make_async_copy(tok_hbm, tok.at[0, own_rows], loc_sem.at[2]),
    )
    for copy in local:
        copy.start()
    for e in range(ng):
        gate_copy(e, e).start(priority=1)
        up_copy(e, e).start(priority=1)
    for k in range(nd):
        down_copy(k, k).start(priority=1)

    barrier = pltpu.get_barrier_semaphore()
    for axis, me, n in (("expert", me_e, n_e), ("dp", me_d, n_d), ("tensor", me_t, n_t)):
        for o in range(1, n):
            pl.semaphore_signal(barrier, inc=1, device_id={axis: lax.rem(me + o, n)}, device_id_type=MESH)
    pl.semaphore_wait(barrier, n_e + n_d + n_t - 3)

    half = width // 2
    mine = pl.ds(pl.multiple_of(lax.rem(me_d, 2) * half, LANES), half)
    theirs = pl.ds(pl.multiple_of((1 - lax.rem(me_d, 2)) * half, LANES), half)
    partner = me_d + 1 - 2 * lax.rem(me_d, 2)
    for copy in local:
        copy.wait()
    ids_out, gw_out, tok_out, rel_out = [], [], [], []
    for o in range(1, n_e):
        to = lax.rem(me_e + o, n_e)
        ids_out.append(remote(ids.at[0], ids.at[o], ids_send.at[o - 1], ids_recv.at[o - 1], expert=to))
        gw_out.append(remote(gw.at[0], gw.at[o], gw_send.at[o - 1], gw_recv.at[o - 1], expert=to))
        tok_out.append(
            remote(
                tok.at[0, own_rows, mine], tok.at[o, own_rows, mine], tok_send.at[o - 1], tok_recv.at[o - 1], expert=to
            )
        )
        rel_out.append(
            remote(
                tok.at[o, own_rows, mine], tok.at[o, own_rows, mine], rel_send.at[o - 1], rel_recv.at[o - 1], dp=partner
            )
        )
    for copy in ids_out + gw_out + tok_out:
        copy.start()

    if t_pad > t_dev:
        for p in range(n_e):
            tok[p, t_dev:t_pad, :] = jnp.zeros((t_pad - t_dev, width), BF16)
    lane = lax.broadcasted_iota(I32, (t_dev, all_slots), 1)
    lane_expert = lane // slots + me_e * experts
    lane_slot = lane % slots
    earlier = (
        lax.broadcasted_iota(I32, (t_dev, t_dev), 1) < lax.broadcasted_iota(I32, (t_dev, t_dev), 0)
    ).astype(F32).astype(BF16)
    picks, weights = [], []
    for p in range(n_e):
        if p > 0:
            ids_out[p - 1].wait_recv()
            gw_out[p - 1].wait_recv()
        named = jnp.zeros((t_dev, all_slots), F32)
        weight = jnp.zeros((t_dev, all_slots), F32)
        ids_p, gw_p = ids[p], gw[p]
        for k in range(top):
            hit = ids_p[:, k : k + 1] == lane_expert
            named = jnp.where(hit, 1.0, named)
            weight = jnp.where(hit, gw_p[:, k : k + 1], weight)
        rank = jnp.dot(earlier, named.astype(BF16), preferred_element_type=F32)
        at = (rank + p * CAP).astype(I32)
        pick = jnp.where(at == lane_slot, named, 0.0)
        rest = jnp.zeros((t_pad - t_dev, all_slots), F32)
        picks += [pick, rest]
        weights += [pick * weight, rest]
    table[...] = jnp.concatenate(picks, axis=0).T.astype(BF16)
    slot_weight = jnp.sum(jnp.concatenate(weights, axis=0).T, axis=1, keepdims=True)
    scale[...] = jnp.broadcast_to(slot_weight, (all_slots, hid))

    for o in range(1, n_e):
        tok_out[o - 1].wait_recv()
        rel_out[o - 1].start()
    for o in range(1, n_e):
        remote(
            tok.at[o, own_rows, theirs], tok.at[o, own_rows, theirs], rel_send.at[o - 1], rel_recv.at[o - 1], dp=partner
        ).wait_recv()

    @pl.loop(0, chunks)
    def _(c):
        cols = pl.ds(pl.multiple_of(c * chunk, LANES), chunk)
        feed = tok[:, :, cols].reshape(n_e * t_pad, chunk)
        rows_x[:, cols] = jnp.dot(table[...], feed, preferred_element_type=F32).astype(BF16)

    def partial_copy(e, o):
        return remote(
            snd.at[e], rcv.at[o - 1, e], gu_send.at[o - 1, e], gu_recv.at[o - 1, e], tensor=lax.rem(me_t + o, n_t)
        )

    def finish_hidden(e):
        total = snd[e]
        for o in range(1, n_t):
            partial_copy(e, o).wait_recv()
            total = total + rcv[o - 1, e]
        gate, up = total[:, :hid], total[:, hid:]
        rows = pl.ds(pl.multiple_of(e * slots, slots), slots)
        hidden = (gate / (1.0 + jnp.exp(-gate)) * up * scale[rows, :]).astype(BF16)
        spread = lax.dot_general(
            table[rows, :], hidden, (((0,), (0,)), ((), ())), preferred_element_type=F32
        )
        if t_pad > t_dev:
            spread = spread.reshape(n_e, t_pad, hid)[:, :t_dev, :].reshape(n_e * t_dev, hid)
        dense[:, pl.ds(pl.multiple_of(e * hid, hid), hid)] = spread.astype(BF16)

    @pl.loop(0, experts)
    def _(e):
        slot = lax.rem(e, ng)
        rows = pl.ds(pl.multiple_of(e * slots, slots), slots)
        x = rows_x[rows, :]
        gate_copy(e, slot).wait()
        gate = jnp.dot(x, wg[slot], preferred_element_type=F32)
        up_copy(e, slot).wait()
        up = jnp.dot(x, wu[slot], preferred_element_type=F32)
        snd[e, :, :hid] = gate
        snd[e, :, hid:] = up

        @pl.when(e + ng < experts)
        def _():
            gate_copy(e + ng, slot).start(priority=1)
            up_copy(e + ng, slot).start(priority=1)

        for o in range(1, n_t):
            partial_copy(e, o).start()

        @pl.when(e >= HIDDEN_LAG)
        def _():
            finish_hidden(e - HIDDEN_LAG)

    @pl.loop(max(experts - HIDDEN_LAG, 0), experts)
    def _(e):
        finish_hidden(e)

    def send_dp(c):
        for o in range(1, n_d):
            d = lax.rem(me_d + o, n_d)
            remote(rs_buf.at[c, d], rs_recv.at[c, o - 1], rs_ssem.at[c], rs_rsem.at[c], dp=d).start()

    def whole_dp(c):
        return remote(rs_buf.at[c, pl.ds(0, n_d - 1)], rs_recv.at[c], rs_ssem.at[c], rs_rsem.at[c], dp=next_d)

    def whole_ex(c):
        return remote(ex_send.at[c, pl.ds(1, n_e - 1)], ex_recv.at[c], ex_ssem.at[c], ex_rsem.at[c], expert=next_e)

    def whole_ag(c):
        span = ag.at[c, pl.ds(0, n_d - 1)]
        return remote(span, span, ag_ssem.at[c], ag_rsem.at[c], dp=next_d)

    def reduce_dp(c):
        whole_dp(c).wait_recv()
        total = rs_buf[c, me_d].astype(F32)
        for o in range(1, n_d):
            total = total + rs_recv[c, o - 1].astype(F32)
        for p in range(n_e):
            ex_send[c, p] = total[p * t_dev : (p + 1) * t_dev, :].astype(BF16)
        for p in range(1, n_e):
            to = lax.rem(me_e + n_e - p, n_e)
            remote(ex_send.at[c, p], ex_recv.at[c, p - 1], ex_ssem.at[c], ex_rsem.at[c], expert=to).start()

    def reduce_ex(c):
        whole_ex(c).wait_recv()
        total = ex_send[c, 0].astype(F32)
        for p in range(1, n_e):
            total = total + ex_recv[c, p - 1].astype(F32)
        ag[c, me_d] = total.astype(BF16)
        for o in range(1, n_d):
            d = lax.rem(me_d + o, n_d)
            remote(ag.at[c, me_d], ag.at[c, me_d], ag_ssem.at[c], ag_rsem.at[c], dp=d).start()

    def finish(c):
        whole_ag(c).wait_recv()
        for q in range(n_d):
            first = c * chunk + q * part
            out_ref[:, first : first + part] = ag[c, q]

    for c in range(chunks):
        slot = c % nd
        down_copy(c, slot).wait()
        acc = jnp.dot(
            dense[...], wd[slot].reshape(experts * hid, chunk), preferred_element_type=F32
        )
        for q in range(n_d):
            rs_buf[c, q] = acc[:, q * part : (q + 1) * part].astype(BF16)
        if c + nd < chunks:
            down_copy(c + nd, slot).start(priority=1)
        send_dp(c)
        if c >= 2:
            reduce_dp(c - 2)
        if c >= 5:
            reduce_ex(c - 5)
    for c in range(max(chunks - 2, 0), chunks):
        reduce_dp(c)
    for c in range(max(chunks - 5, 0), chunks):
        reduce_ex(c)
    for c in range(chunks):
        finish(c)

    for copy in ids_out + gw_out + tok_out + rel_out:
        copy.wait_send()

    @pl.loop(0, experts)
    def _(e):
        for o in range(1, n_t):
            partial_copy(e, o).wait_send()

    for c in range(chunks):
        whole_dp(c).wait_send()
        whole_ex(c).wait_send()
        whole_ag(c).wait_send()


def per_device(cfg, tokens, expert_ids, gate_weights, w_gate, w_up, w_down):
    n_e, n_d, n_t = cfg["n_e"], cfg["n_d"], cfg["n_t"]
    t_dev, width = tokens.shape
    top = expert_ids.shape[1]
    experts, _, hid = w_gate.shape
    t_pad = -(-t_dev // 16) * 16
    chunk = n_d * LANES
    while width % chunk:
        chunk -= LANES
    chunks = width // chunk
    nd = min(DOWN_SLOTS, chunks)
    room = WEIGHT_VMEM - nd * experts * hid * chunk * 2
    ng = max(1, min(experts, room // (width * hid * 4)))
    part = chunk // n_d
    slots = n_e * CAP
    cfg = dict(
        cfg, experts=experts, width=width, hid=hid, t_dev=t_dev, t_pad=t_pad, top=top,
        ng=ng, nd=nd, chunk=chunk, chunks=chunks,
    )
    dma, vmem = pltpu.SemaphoreType.DMA, pltpu.VMEM
    scratch = [
        vmem((ng, width, hid), BF16),
        vmem((ng, width, hid), BF16),
        vmem((nd, experts, hid, chunk), BF16),
        vmem((n_e, t_pad, width), BF16),
        vmem((n_e, t_dev, top), I32),
        vmem((n_e, t_dev, top), F32),
        vmem((experts * slots, n_e * t_pad), BF16),
        vmem((experts * slots, hid), F32),
        vmem((experts * slots, width), BF16),
        vmem((experts, slots, 2 * hid), F32),
        vmem((n_t - 1, experts, slots, 2 * hid), F32),
        vmem((n_e * t_dev, experts * hid), BF16),
        vmem((chunks, n_d, n_e * t_dev, part), BF16),
        vmem((chunks, n_d - 1, n_e * t_dev, part), BF16),
        vmem((chunks, n_e, t_dev, part), BF16),
        vmem((chunks, n_e - 1, t_dev, part), BF16),
        vmem((chunks, n_d, t_dev, part), BF16),
        dma((2, ng)), dma((nd,)), dma((3,)),
        dma((n_e - 1,)), dma((n_e - 1,)), dma((n_e - 1,)), dma((n_e - 1,)),
        dma((n_e - 1,)), dma((n_e - 1,)), dma((n_e - 1,)), dma((n_e - 1,)),
        dma((n_t - 1, experts)), dma((n_t - 1, experts)),
        dma((chunks,)), dma((chunks,)), dma((chunks,)), dma((chunks,)), dma((chunks,)), dma((chunks,)),
    ]
    anywhere = pl.BlockSpec(memory_space=pl.ANY)
    return pl.pallas_call(
        functools.partial(layer_kernel, cfg),
        out_shape=jax.ShapeDtypeStruct((t_dev, width), BF16),
        in_specs=[anywhere] * 6,
        out_specs=pl.BlockSpec(memory_space=vmem),
        scratch_shapes=scratch,
        compiler_params=pltpu.CompilerParams(
            collective_id=0, has_side_effects=True, vmem_limit_bytes=VMEM_LIMIT
        ),
    )(tokens, expert_ids, gate_weights, w_gate, w_up, w_down)


def solution(mesh):
    cfg = {"n_e": mesh.shape["expert"], "n_d": mesh.shape["dp"], "n_t": mesh.shape["tensor"]}
    in_specs = (
        P("expert", "tensor"),
        P("expert", None),
        P("expert", None),
        P("expert", "tensor", "dp"),
        P("expert", "tensor", "dp"),
        P("expert", "dp", "tensor"),
    )
    return jax.shard_map(
        functools.partial(per_device, cfg), mesh=mesh, in_specs=in_specs,
        out_specs=P("expert", "tensor"), check_vma=False,
    )
```
